8 devices in a mesh: dp: 1 (over z), sh: 8 (over y, x, core).
Axes of the slice: x: 2, y: 2, z: 1, core: 2. Of those that a mesh axis runs over, the one named last changes fastest.
Arguments:
- k_prefill: bfloat16 [16, 5120, 16, 128], P('dp', None, 'sh')
- v_prefill: bfloat16 [16, 5120, 16, 128], P('dp', None, 'sh')
- lengths: int32 [16], P('dp')
- residual: bfloat16 [16, 4608], P(('dp', 'sh'))
- norm_gain: bfloat16 [4608], replicated
- w_query: bfloat16 [4608, 4096], replicated
- w_key: bfloat16 [4608, 2048], replicated
- w_value: bfloat16 [4608, 2048], replicated
- w_out: bfloat16 [4096, 4608], replicated
Outputs:
- output 1: bfloat16 [16, 4608], P(('dp', 'sh'))
- output 2: bfloat16 [16, 4096, 16, 128], P(('dp', 'sh'))
- output 3: bfloat16 [16, 4096, 16, 128], P(('dp', 'sh'))
All inputs are finite; a program needn't handle non-finite values.
Results may differ from the reference program's by a relative error of at most 0.00409.
Values are sent between devices in bfloat16 or wider.
A program may use at most 1 GiB of HBM per device.

```python
import jax
import jax.numpy as jnp
from jax import lax

MODEL_DIM = 4608
HEADS = 32
KV_HEADS = 16
HEAD_DIM = 128
WINDOW = 4096
SEQ_LEN = 5120
BATCH = 16
Q_GROUP = HEADS // KV_HEADS
Q_WIDTH = HEADS * HEAD_DIM
KV_WIDTH = KV_HEADS * HEAD_DIM
THETA = 10000.0
EPS = 1e-5


def setup_inputs(seed: int = 0, part: int = 0) -> dict:
    root_key = jax.random.key(seed)
    part_root, shared_root = jax.random.split(root_key)
    part_keys = jax.random.split(jax.random.fold_in(part_root, part), 4)
    shared_keys = jax.random.split(shared_root, 5)
    kv_shape = (BATCH, SEQ_LEN, KV_HEADS, HEAD_DIM)
    k_prefill = jax.random.normal(part_keys[0], kv_shape, jnp.float32).astype(jnp.bfloat16)
    v_prefill = jax.random.normal(part_keys[1], kv_shape, jnp.float32).astype(jnp.bfloat16)
    lengths = jax.random.randint(part_keys[2], (BATCH,), 1, SEQ_LEN + 1, dtype=jnp.int32)
    lengths = lengths.at[0].set(SEQ_LEN).at[1].set(1)
    residual = jax.random.normal(part_keys[3], (BATCH, MODEL_DIM), jnp.float32).astype(jnp.bfloat16)
    norm_gain = (1.0 + 0.3 * jax.random.normal(shared_keys[0], (MODEL_DIM,), jnp.float32)).astype(jnp.bfloat16)
    w_query = (jax.random.normal(shared_keys[1], (MODEL_DIM, Q_WIDTH), jnp.float32) * (2.0 / MODEL_DIM ** 0.5)).astype(jnp.bfloat16)
    w_key = (jax.random.normal(shared_keys[2], (MODEL_DIM, KV_WIDTH), jnp.float32) * (3.0 / MODEL_DIM ** 0.5)).astype(jnp.bfloat16)
    w_value = (jax.random.normal(shared_keys[3], (MODEL_DIM, KV_WIDTH), jnp.float32) * (3.0 / MODEL_DIM ** 0.5)).astype(jnp.bfloat16)
    w_out = (jax.random.normal(shared_keys[4], (Q_WIDTH, MODEL_DIM), jnp.float32) * (2.0 / Q_WIDTH ** 0.5)).astype(jnp.bfloat16)
    return {'k_prefill': k_prefill, 'v_prefill': v_prefill, 'lengths': lengths, 'residual': residual, 'norm_gain': norm_gain, 'w_query': w_query, 'w_key': w_key, 'w_value': w_value, 'w_out': w_out}


def rolling_cache(prefill, lengths):
    slot_ids = jnp.arange(WINDOW, dtype=jnp.int32)
    last_pos = lengths[:, None] - 1
    held_pos = last_pos - jnp.remainder(last_pos - slot_ids[None, :], WINDOW)
    held = jax.vmap(lambda row_vals, row_idx: jnp.take(row_vals, row_idx, axis=0))(prefill, jnp.maximum(held_pos, 0))
    return jnp.where((held_pos >= 0)[:, :, None, None], held, jnp.zeros((), prefill.dtype))


def rotate(heads, positions):
    half_dim = HEAD_DIM // 2
    inv_freq = THETA ** (-2.0 * jnp.arange(half_dim, dtype=jnp.float32) / HEAD_DIM)
    angles = positions.astype(jnp.float32).reshape(positions.shape + (1,) * (heads.ndim - 1)) * inv_freq
    cos_part = jnp.cos(angles)
    sin_part = jnp.sin(angles)
    first_half = heads[..., :half_dim].astype(jnp.float32)
    second_half = heads[..., half_dim:].astype(jnp.float32)
    return jnp.concatenate([first_half * cos_part - second_half * sin_part, second_half * cos_part + first_half * sin_part], axis=-1).astype(jnp.bfloat16)


def attend_row(row_args):
    q_row, k_row, v_row, live_row = row_args
    q_grouped = q_row.reshape(KV_HEADS, Q_GROUP, HEAD_DIM).astype(jnp.float32)
    scores = jnp.einsum('kgd,wkd->kgw', q_grouped, k_row.astype(jnp.float32)) / HEAD_DIM ** 0.5
    scores = jnp.where(live_row[None, None, :], scores, -jnp.inf)
    weights = jax.nn.softmax(scores, axis=-1).astype(jnp.bfloat16)
    mixed = jnp.einsum('kgw,wkd->kgd', weights.astype(jnp.float32), v_row.astype(jnp.float32))
    return mixed.astype(jnp.bfloat16).reshape(Q_WIDTH)


def reference(k_prefill, v_prefill, lengths, residual, norm_gain, w_query, w_key, w_value, w_out):
    k_cache = rolling_cache(k_prefill, lengths)
    v_cache = rolling_cache(v_prefill, lengths)
    resid_f32 = residual.astype(jnp.float32)
    inv_rms = lax.rsqrt(jnp.mean(resid_f32 * resid_f32, axis=-1, keepdims=True) + EPS)
    normed = (resid_f32 * inv_rms * norm_gain.astype(jnp.float32)).astype(jnp.bfloat16)
    q_heads = jnp.dot(normed, w_query, preferred_element_type=jnp.float32).astype(jnp.bfloat16).reshape(BATCH, HEADS, HEAD_DIM)
    k_new = jnp.dot(normed, w_key, preferred_element_type=jnp.float32).astype(jnp.bfloat16).reshape(BATCH, KV_HEADS, HEAD_DIM)
    v_new = jnp.dot(normed, w_value, preferred_element_type=jnp.float32).astype(jnp.bfloat16).reshape(BATCH, KV_HEADS, HEAD_DIM)
    q_heads = rotate(q_heads, lengths)
    k_new = rotate(k_new, lengths)
    slot_ids = jnp.arange(WINDOW, dtype=jnp.int32)
    new_slot = (slot_ids[None, :] == (lengths % WINDOW)[:, None])[:, :, None, None]
    k_cache = jnp.where(new_slot, k_new[:, None], k_cache)
    v_cache = jnp.where(new_slot, v_new[:, None], v_cache)
    live_slot = (lengths[:, None] - jnp.remainder(lengths[:, None] - slot_ids[None, :], WINDOW)) >= 0
    attn_out = lax.map(attend_row, (q_heads, k_cache, v_cache, live_slot))
    resid_out = (resid_f32 + jnp.dot(attn_out, w_out, preferred_element_type=jnp.float32)).astype(jnp.bfloat16)
    return (resid_out, k_cache, v_cache)
```

```python
import functools

import jax
import jax.numpy as jnp
from jax import lax
from jax.experimental import pallas as pl
from jax.experimental.pallas import tpu as pltpu
from jax.sharding import PartitionSpec as P

WINDOW = 4096
SEQ = 5120
BATCH = 16
KVH = 16
HD = 128
THETA = 10000.0
EPS = 1e-5
MESH = pl.DeviceIdType.MESH

BLK = 128
NBLK = WINDOW // BLK
CHIP_ROWS = 4
STREAM = CHIP_ROWS * NBLK
BIG = 4
LEVELS = tuple(range(36, STREAM + 1, 4))
CHUNKS = 6


def row_blocks(n):
    return (jnp.minimum(n, WINDOW) + (BLK - 1)) // BLK


RING = 16
DEPTH = 8
MAXBIG = BATCH * NBLK // BIG + 16
MAXSMALL = BATCH * 2 * BIG


def pack_kernel(len_ref, k_ref, v_ref, sk_ref, sv_ref, bsrc, bdst, ssrc, sdst,
                kbuf, vbuf, mixk, mixv, in_sem, out_sem, mix_in, mix_out):
    row_pos = SEQ // BLK

    def is_mixed(n):
        return jnp.logical_and(n > WINDOW, n % BLK != 0)

    def mix_copies(b, n):
        first = jnp.maximum(n - WINDOW, 0) // BLK
        src = (b * row_pos + first) * BLK
        out = []
        for x, (ref, buf) in enumerate(((k_ref, mixk), (v_ref, mixv))):
            for half in range(2):
                start = jnp.minimum(src + half * WINDOW, BATCH * SEQ - BLK)
                out.append(pltpu.make_async_copy(
                    ref.at[pl.ds(start, BLK)], buf.at[b, half], mix_in.at[b, x, half]))
        return out

    def row(b, carry):
        nbig, nsmall, start = carry
        start = jnp.where(b % CHIP_ROWS == 0, (b // CHIP_ROWS) * STREAM, start)
        n = len_ref[b]
        nb = row_blocks(n)
        first = jnp.maximum(n - WINDOW, 0) // BLK
        mixed = is_mixed(n)

        @pl.when(mixed)
        def _():
            for c in mix_copies(b, n):
                c.start()

        def segment(lo, hi, shift, counts):
            nbig, nsmall = counts
            big = (hi - lo) // BIG
            small = (hi - lo) - big * BIG

            def put_big(i, _):
                at = lo + i * BIG
                bsrc[nbig + i] = b * row_pos + at + shift
                bdst[nbig + i] = start + at
                return 0

            def put_small(i, _):
                at = lo + big * BIG + i
                ssrc[nsmall + i] = b * row_pos + at + shift
                sdst[nsmall + i] = start + at
                return 0
            lax.fori_loop(0, big, put_big, 0)
            lax.fori_loop(0, small, put_small, 0)
            return nbig + big, nsmall + small
        counts = segment(jnp.int32(0), first, NBLK, (nbig, nsmall))
        counts = segment(first + mixed.astype(jnp.int32), nb, 0, counts)
        return counts[0], counts[1], start + nb

    zero = jnp.int32(0)
    nbig, nsmall, _ = lax.fori_loop(0, BATCH, row, (zero, zero, zero))

    def run(count, src_tab, dst_tab, blocks):
        size = blocks * BLK

        def ins(i):
            slot = i % RING
            src = pl.ds(src_tab[i] * BLK, size)
            return [pltpu.make_async_copy(r.at[src], buf.at[slot, pl.ds(0, size)], in_sem.at[slot, x])
                    for x, (r, buf) in enumerate(((k_ref, kbuf), (v_ref, vbuf)))]

        def outs(i):
            slot = i % RING
            dst = pl.ds(dst_tab[i] * BLK, size)
            return [pltpu.make_async_copy(buf.at[slot, pl.ds(0, size)], r.at[dst], out_sem.at[slot, x])
                    for x, (r, buf) in enumerate(((sk_ref, kbuf), (sv_ref, vbuf)))]

        def step(i, _):
            @pl.when(i < count)
            def _():
                @pl.when(i >= RING)
                def _():
                    for c in outs(i - RING):
                        c.wait()
                for c in ins(i):
                    c.start()
            j = i - DEPTH

            @pl.when(jnp.logical_and(j >= 0, j < count))
            def _():
                for c in ins(j):
                    c.wait()
                for c in outs(j):
                    c.start()
            return 0
        lax.fori_loop(0, count + DEPTH, step, 0)

        def drain(i, _):
            for c in outs(i):
                c.wait()
            return 0
        lax.fori_loop(jnp.maximum(count - RING, 0), count, drain, 0)

    run(nbig, bsrc, bdst, BIG)
    run(nsmall, ssrc, sdst, 1)

    def mix_out_copies(b, n, start):
        dst = pl.ds((start + jnp.maximum(n - WINDOW, 0) // BLK) * BLK, BLK)
        return [pltpu.make_async_copy(buf.at[b, 0], ref.at[dst], mix_out.at[b, x])
                for x, (ref, buf) in enumerate(((sk_ref, mixk), (sv_ref, mixv)))]

    def mix_row(b, start):
        start = jnp.where(b % CHIP_ROWS == 0, (b // CHIP_ROWS) * STREAM, start)
        n = len_ref[b]

        @pl.when(is_mixed(n))
        def _():
            for c in mix_copies(b, n):
                c.wait()
            wrapped = lax.broadcasted_iota(jnp.int32, (BLK, 2, HD), 0) < n % BLK
            for buf in (mixk, mixv):
                buf[b, 0] = jnp.where(wrapped, buf[b, 1], buf[b, 0])
            for c in mix_out_copies(b, n, start):
                c.start()
        return start + row_blocks(n)

    def mix_wait(b, start):
        start = jnp.where(b % CHIP_ROWS == 0, (b // CHIP_ROWS) * STREAM, start)
        n = len_ref[b]

        @pl.when(is_mixed(n))
        def _():
            for c in mix_out_copies(b, n, start):
                c.wait()
        return start + row_blocks(n)
    lax.fori_loop(0, BATCH, mix_row, zero)
    lax.fori_loop(0, BATCH, mix_wait, zero)


def pack(lengths, k, v):
    out = jax.ShapeDtypeStruct((4 * STREAM * BLK, 2, HD), jnp.bfloat16)
    hbm = pl.BlockSpec(memory_space=pl.ANY)
    return pl.pallas_call(
        pack_kernel,
        out_shape=(out, out),
        in_specs=[pl.BlockSpec(memory_space=pltpu.SMEM), hbm, hbm],
        out_specs=(hbm, hbm),
        scratch_shapes=[
            pltpu.SMEM((MAXBIG,), jnp.int32), pltpu.SMEM((MAXBIG,), jnp.int32),
            pltpu.SMEM((MAXSMALL,), jnp.int32), pltpu.SMEM((MAXSMALL,), jnp.int32),
            pltpu.VMEM((RING, BIG * BLK, 2, HD), jnp.bfloat16),
            pltpu.VMEM((RING, BIG * BLK, 2, HD), jnp.bfloat16),
            pltpu.VMEM((BATCH, 2, BLK, 2, HD), jnp.bfloat16),
            pltpu.VMEM((BATCH, 2, BLK, 2, HD), jnp.bfloat16),
            pltpu.SemaphoreType.DMA((RING, 2)), pltpu.SemaphoreType.DMA((RING, 2)),
            pltpu.SemaphoreType.DMA((BATCH, 2, 2)), pltpu.SemaphoreType.DMA((BATCH, 2)),
        ],
        name="pack",
    )(lengths, k.reshape(BATCH * SEQ, 2, HD), v.reshape(BATCH * SEQ, 2, HD))


def exchange_kernel(nblk, sk_ref, sv_ref, rk_ref, rv_ref,
                    send_sem, recv_sem, fsend_sem, frecv_sem, own_sem):
    me = lax.axis_index("sh")
    core = me % 2
    chip_x = (me // 2) % 2
    chip_y = me // 4
    partner = me + 1 - 2 * core
    chips = (chip_y * 2 + (1 - chip_x), (1 - chip_y) * 2 + chip_x, (1 - chip_y) * 2 + (1 - chip_x))
    peers = [c * 2 + core for c in chips]
    my_chip = me // 2

    barrier = pltpu.get_barrier_semaphore()
    for p in peers + [partner]:
        pl.semaphore_signal(barrier, inc=1, device_id={"sh": p}, device_id_type=MESH)
    pl.semaphore_wait(barrier, 4)

    edges = [nblk * i // CHUNKS for i in range(CHUNKS + 1)]
    chunks = [(src, dst, edges[i] * BLK, (edges[i + 1] - edges[i]) * BLK)
              for src, dst in ((sk_ref, rk_ref), (sv_ref, rv_ref)) for i in range(CHUNKS)]
    base = STREAM * BLK

    def send(t, j):
        src, dst, lo, size = chunks[t]
        return pltpu.make_async_remote_copy(
            src.at[pl.ds(chips[j] * base + lo, size)], dst.at[pl.ds(lo, size), me],
            send_sem.at[j, t], recv_sem.at[j, t], device_id={"sh": peers[j]}, device_id_type=MESH)

    def forward(t, j):
        _, dst, lo, size = chunks[t]
        view = dst.at[pl.ds(lo, size), peers[j]]
        return pltpu.make_async_remote_copy(
            view, view, fsend_sem.at[j, t], frecv_sem.at[j, t],
            device_id={"sh": partner}, device_id_type=MESH)

    total = len(chunks)
    ahead = 2
    sends = [[send(t, j) for j in range(3)] for t in range(total)]
    forwards = [[forward(t, j) for j in range(3)] for t in range(total)]
    for t in range(ahead):
        for c in sends[t]:
            c.start()
    own = []
    for x, (src, dst) in enumerate(((sk_ref, rk_ref), (sv_ref, rv_ref))):
        mine = src.at[pl.ds(my_chip * base, nblk * BLK)]
        view = dst.at[pl.ds(0, nblk * BLK), me]
        own.append(pltpu.make_async_copy(mine, view, own_sem.at[x]))
        own.append(pltpu.make_async_remote_copy(
            mine, view, fsend_sem.at[3, x], frecv_sem.at[3, x],
            device_id={"sh": partner}, device_id_type=MESH))
    for c in own:
        c.start()
    for t in range(total):
        for c in sends[t]:
            c.wait_send()
        if t + ahead < total:
            for c in sends[t + ahead]:
                c.start()
        for j in range(3):
            sends[t][j].wait_recv()
            forwards[t][j].start()
    for c in own:
        c.wait()
    for t in range(total):
        for c in forwards[t]:
            c.wait()


def exchange(level, sk, sv):
    out = jax.ShapeDtypeStruct((STREAM * BLK, 8, 2, HD), jnp.bfloat16)
    hbm = pl.BlockSpec(memory_space=pl.ANY)
    total = 2 * CHUNKS

    def branch(i, sk, sv):
        return pl.pallas_call(
            functools.partial(exchange_kernel, LEVELS[i]),
            out_shape=(out, out),
            in_specs=[hbm, hbm],
            out_specs=(hbm, hbm),
            scratch_shapes=[
                pltpu.SemaphoreType.DMA((3, total)), pltpu.SemaphoreType.DMA((3, total)),
                pltpu.SemaphoreType.DMA((4, total)), pltpu.SemaphoreType.DMA((4, total)),
                pltpu.SemaphoreType.DMA((2,)),
            ],
            compiler_params=pltpu.CompilerParams(collective_id=i, has_side_effects=True),
            name=f"exchange_{LEVELS[i]}",
        )(sk, sv)
    return lax.switch(level, [functools.partial(branch, i) for i in range(len(LEVELS))], sk, sv)


NBUF = 8
LOOK = 5
COLS = BLK * KVH


def attend_kernel(len_ref, q_ref, kn_ref, vn_ref, rk_ref, rv_ref, o_ref, kc_ref, vc_ref,
                  buf, zbuf, sc, mx, acc, in_sem, out_sem, zero_sem):
    me = lax.axis_index("sh")
    row0 = 2 * me
    base = CHIP_ROWS * (me // 2)
    lens = [len_ref[row0], len_ref[row0 + 1]]
    before = row_blocks(len_ref[base]) + row_blocks(len_ref[base + 1])
    start0 = jnp.where(me % 2 == 1, before, 0)
    starts = [start0, start0 + row_blocks(lens[0])]
    acts = [jnp.where(n >= WINDOW, NBLK, n // BLK + 1) for n in lens]
    units = acts[0] + acts[1]

    def where_is(u):
        second = u >= acts[0]
        r = second.astype(jnp.int32)
        sig = jnp.where(second, u - acts[0], u)
        beta = jnp.where(second, starts[1], starts[0]) + sig
        return r, sig, beta, jnp.where(second, lens[1], lens[0])

    def in_copy(ref, w, u):
        _, _, beta, _ = where_is(u)
        return pltpu.make_async_copy(ref.at[pl.ds(beta * BLK, BLK)], buf.at[w % NBUF], in_sem.at[w % NBUF])

    def out_copy(ref, w, u):
        r, sig, _, _ = where_is(u)
        return pltpu.make_async_copy(buf.at[w % NBUF], ref.at[r, pl.ds(sig * BLK, BLK)], out_sem.at[w % NBUF])

    def start_in(w):
        @pl.when(w < units)
        def _():
            in_copy(rk_ref, w, w).start()

        @pl.when(jnp.logical_and(w >= units, w < 2 * units))
        def _():
            in_copy(rv_ref, w, w - units).start()

    def wait_out(w):
        @pl.when(w >= 0)
        def _():
            out_copy(kc_ref, w, 0).wait()

    for w in range(LOOK):
        start_in(jnp.int32(w))

    zbuf[...] = jnp.zeros_like(zbuf)

    def zero_copies(r, sig):
        return [pltpu.make_async_copy(zbuf, ref.at[r, pl.ds(sig * BLK, BLK)], zero_sem.at[x])
                for x, ref in enumerate((kc_ref, vc_ref))]
    for r in range(2):
        def put_zero(sig, _, r=r):
            for c in zero_copies(r, sig):
                c.start()
            return 0
        lax.fori_loop(acts[r], NBLK, put_zero, 0)

    mx[...] = jnp.full_like(mx, -jnp.inf)
    acc[...] = jnp.zeros_like(acc)
    col = lax.broadcasted_iota(jnp.int32, (32, COLS), 1)
    rowid = lax.broadcasted_iota(jnp.int32, (32, COLS), 0)
    match = (rowid % KVH) == (col % KVH)
    col2 = lax.broadcasted_iota(jnp.int32, (2, COLS), 1) // KVH
    scale = 1.0 / HD ** 0.5

    def fix(slot, r, sig, n, new_ref):
        new_slot = n % WINDOW

        @pl.when(sig == new_slot // BLK)
        def _():
            here = sig * BLK + lax.broadcasted_iota(jnp.int32, (BLK, KVH, HD), 0)
            val = buf[slot]
            val = jnp.where(here > n, jnp.zeros_like(val), val)
            new = jnp.broadcast_to(new_ref[r][None], val.shape)
            buf[slot] = jnp.where(here == new_slot, new, val)

    def k_step(u, _):
        r, sig, _, n = where_is(u)
        slot = u % NBUF
        wait_out(u + LOOK - NBUF)
        start_in(u + LOOK)
        in_copy(rk_ref, u, u).wait()
        fix(slot, r, sig, n, kn_ref)
        kb = buf[slot].reshape(COLS, HD)
        s = lax.dot_general(q_ref[r], kb, (((1,), (1,)), ((), ())), preferred_element_type=jnp.float32)
        out_copy(kc_ref, u, u).start()
        s = jnp.where(match, s, 0.0)
        s = jnp.concatenate([jnp.sum(s[:KVH], axis=0, keepdims=True),
                             jnp.sum(s[KVH:], axis=0, keepdims=True)], axis=0)
        s = jnp.where(sig * BLK + col2 > n, -jnp.inf, s * scale)
        sc[u] = s
        mx[r] = jnp.maximum(mx[r], s)
        return 0
    lax.fori_loop(0, units, k_step, 0)

    def fold(x, op):
        y = x[:, :HD]
        for i in range(1, COLS // HD):
            y = op(y, x[:, i * HD:(i + 1) * HD])
        for sh in (16, 32, 64):
            y = op(y, pltpu.roll(y, sh, 1))
        return jnp.concatenate([y] * (COLS // HD), axis=1)

    for r in range(2):
        top = fold(mx[r], jnp.maximum)
        lo = 0 if r == 0 else acts[0]

        def exp_step(i, tot, top=top, lo=lo):
            e = jnp.exp(sc[lo + i] - top)
            sc[lo + i] = e
            return tot + e
        tot = lax.fori_loop(0, acts[r], exp_step, jnp.zeros((2, COLS), jnp.float32))
        mx[r] = fold(tot, jnp.add)

    def v_step(u, _):
        r, sig, _, n = where_is(u)
        w = u + units
        slot = w % NBUF
        wait_out(w + LOOK - NBUF)
        start_in(w + LOOK)
        in_copy(rv_ref, w, u).wait()
        fix(slot, r, sig, n, vn_ref)
        p = sc[u] / mx[r]
        wide = jnp.concatenate([jnp.broadcast_to(p[0:1], (KVH, COLS)),
                                jnp.broadcast_to(p[1:2], (KVH, COLS))], axis=0)
        wide = jnp.where(match, wide, 0.0).astype(jnp.bfloat16)
        vb = buf[slot].reshape(COLS, HD)
        acc[r] += jnp.dot(wide, vb, preferred_element_type=jnp.float32)
        out_copy(vc_ref, w, u).start()
        return 0
    lax.fori_loop(0, units, v_step, 0)
    o_ref[...] = acc[...].astype(o_ref.dtype)

    def drain(w, _):
        wait_out(w)
        return 0
    lax.fori_loop(2 * units + LOOK - NBUF, 2 * units, drain, 0)
    for r in range(2):
        def wait_zero(sig, _, r=r):
            for c in zero_copies(r, sig):
                c.wait()
            return 0
        lax.fori_loop(acts[r], NBLK, wait_zero, 0)


def attend(lengths, q, kn, vn, rk, rv):
    hbm = pl.BlockSpec(memory_space=pl.ANY)
    vmem = pl.BlockSpec(memory_space=pltpu.VMEM)
    cache = jax.ShapeDtypeStruct((2, WINDOW, KVH, HD), jnp.bfloat16)
    return pl.pallas_call(
        attend_kernel,
        out_shape=(jax.ShapeDtypeStruct((2, 32, HD), jnp.bfloat16), cache, cache),
        in_specs=[pl.BlockSpec(memory_space=pltpu.SMEM), vmem, vmem, vmem, hbm, hbm],
        out_specs=(vmem, hbm, hbm),
        scratch_shapes=[
            pltpu.VMEM((NBUF, BLK, KVH, HD), jnp.bfloat16),
            pltpu.VMEM((BLK, KVH, HD), jnp.bfloat16),
            pltpu.VMEM((2 * NBLK, 2, COLS), jnp.float32),
            pltpu.VMEM((2, 2, COLS), jnp.float32),
            pltpu.VMEM((2, 32, HD), jnp.float32),
            pltpu.SemaphoreType.DMA((NBUF,)), pltpu.SemaphoreType.DMA((NBUF,)),
            pltpu.SemaphoreType.DMA((2,)),
        ],
        name="attend",
    )(lengths, q, kn, vn, rk.reshape(STREAM * BLK, KVH, HD), rv.reshape(STREAM * BLK, KVH, HD))


def rotate(heads, positions):
    half = HD // 2
    inv_freq = THETA ** (-2.0 * jnp.arange(half, dtype=jnp.float32) / HD)
    angles = positions.astype(jnp.float32).reshape(positions.shape + (1,) * (heads.ndim - 1)) * inv_freq
    cos_part = jnp.cos(angles)
    sin_part = jnp.sin(angles)
    first = heads[..., :half].astype(jnp.float32)
    second = heads[..., half:].astype(jnp.float32)
    return jnp.concatenate([first * cos_part - second * sin_part, second * cos_part + first * sin_part], axis=-1).astype(jnp.bfloat16)


def solution(mesh):
    head_spec = P('dp', None, 'sh', None)
    row_spec = P(('dp', 'sh'))
    full_spec = P(None, None)

    def per_device(k_prefill, v_prefill, lengths, residual, norm_gain, w_query, w_key, w_value, w_out):
        rows = residual.shape[0]
        mine = lax.dynamic_slice_in_dim(lengths, lax.axis_index('sh') * rows, rows)
        longest = jnp.max(jnp.sum(row_blocks(lengths).reshape(4, CHIP_ROWS), axis=1))
        level = jnp.sum(longest > jnp.asarray(LEVELS, jnp.int32)).astype(jnp.int32)

        sk, sv = pack(lengths, k_prefill, v_prefill)
        rk, rv = exchange(level, sk, sv)

        resid = residual.astype(jnp.float32)
        inv_rms = lax.rsqrt(jnp.mean(resid * resid, axis=-1, keepdims=True) + EPS)
        normed = (resid * inv_rms * norm_gain.astype(jnp.float32)).astype(jnp.bfloat16)
        dot = functools.partial(jnp.dot, preferred_element_type=jnp.float32)
        q = dot(normed, w_query).astype(jnp.bfloat16).reshape(rows, KVH, 2, HD)
        kn = dot(normed, w_key).astype(jnp.bfloat16).reshape(rows, KVH, HD)
        vn = dot(normed, w_value).astype(jnp.bfloat16).reshape(rows, KVH, HD)
        q = rotate(q, mine).transpose(0, 2, 1, 3).reshape(rows, 2 * KVH, HD)
        kn = rotate(kn, mine)
        o, kc, vc = attend(lengths, q, kn, vn, rk, rv)
        o = o.reshape(rows, 2, KVH, HD).transpose(0, 2, 1, 3).reshape(rows, 2 * KVH * HD)
        out = (resid + dot(o, w_out)).astype(jnp.bfloat16)
        return out, kc, vc
    return jax.shard_map(per_device, mesh=mesh, in_specs=(head_spec, head_spec, P('dp'), P(('dp', 'sh'), None), P(None), full_spec, full_spec, full_spec, full_spec), out_specs=(P(('dp', 'sh'), None), row_spec, row_spec), check_vma=False)
```

```python
import functools

import jax
import jax.numpy as jnp
from jax import lax
from jax.experimental import pallas as pl
from jax.experimental.pallas import tpu as pltpu
from jax.sharding import PartitionSpec as P

WINDOW = 4096
SEQ = 5120
BATCH = 16
KVH = 16
HD = 128
THETA = 10000.0
EPS = 1e-5
MESH = pl.DeviceIdType.MESH

BLK = 128
NBLK = WINDOW // BLK
CHIP_ROWS = 4
GRAIN = 32
GRAINS = CHIP_ROWS * WINDOW // GRAIN
CSLOTS = 256
MAXCHUNKS = CHIP_ROWS * WINDOW // CSLOTS
LEVELS = (24, 30, 34) + tuple(range(37, 60)) + (61, MAXCHUNKS)
AHEAD = 8
ARRIVE = 32
LAGS = (0, 2, 3, 7)
WCOLS = 256
WBUF = 4
WPART = 8
KSTEP = 512


def row_grains(n):
    return (jnp.minimum(n, WINDOW) + (GRAIN - 1)) // GRAIN


def source_table(lengths):
    n = lengths.reshape(4, CHIP_ROWS)
    count = row_grains(n)
    grain = jnp.arange(GRAINS, dtype=jnp.int32)[None, :]
    begin = jnp.zeros((4, 1), jnp.int32)
    at = grain
    place = jnp.zeros((4, GRAINS), jnp.int32)
    length = n[:, 0:1]
    for r in range(1, CHIP_ROWS):
        begin = begin + count[:, r - 1:r]
        after = grain >= begin
        at = jnp.where(after, grain - begin, at)
        place = jnp.where(after, r * SEQ, place)
        length = jnp.where(after, n[:, r:r + 1], length)
    at = jnp.minimum(at * GRAIN, WINDOW - GRAIN)
    wrapped = jnp.clip(length - WINDOW - at, 0, GRAIN)
    return ((place + at) * 64 + wrapped).reshape(-1)


def exchange_kernel(steps, tab_ref, x_ref, g_ref, k_ref, v_ref, wq_ref, wk_ref, wv_ref,
                    r_ref, p_ref, rows0, rows1, rows2, rows3, stage, wbuf, normed,
                    load_sem, send_sem, recv_sem, own_sem, fsend_sem, frecv_sem, w_sem):
    me = lax.axis_index("sh")
    core = lax.rem(me, 2)
    my_chip = lax.div(me, 2)
    chip_x = lax.rem(my_chip, 2)
    chip_y = lax.div(my_chip, 2)
    partner = me + 1 - 2 * core
    chips = ((1 - chip_y) * 2 + (1 - chip_x), (1 - chip_y) * 2 + chip_x, chip_y * 2 + (1 - chip_x), my_chip)
    peers = [c * 2 + core for c in chips]
    rows = (rows0, rows1, rows2, rows3)
    total = 2 * steps

    def load(ref, j):
        flat = CHIP_ROWS * SEQ
        return pltpu.make_async_copy(ref.at[pl.ds(chips[j] * flat, flat)], rows[j], load_sem.at[j])

    load(k_ref, 0).start()
    barrier = pltpu.get_barrier_semaphore()
    for p in peers[:3] + [partner]:
        pl.semaphore_signal(barrier, inc=1, device_id={"sh": p}, device_id_type=MESH)
    pl.semaphore_wait(barrier, 4)

    def place(c):
        phase = (c >= steps).astype(jnp.int32)
        return phase, pl.ds((c - phase * steps) * CSLOTS, CSLOTS), lax.rem(c, AHEAD)

    def send(c, j):
        phase, slots, slot = place(c)
        return pltpu.make_async_remote_copy(
            stage.at[j, slot], r_ref.at[phase, slots, me], send_sem.at[j, slot], recv_sem.at[j, lax.rem(c, ARRIVE)],
            device_id={"sh": peers[j]}, device_id_type=MESH)

    def own(c):
        phase, slots, slot = place(c)
        return pltpu.make_async_copy(stage.at[3, slot], r_ref.at[phase, slots, me], own_sem.at[slot])

    def forward(c, j):
        phase, slots, _ = place(c)
        view = r_ref.at[phase, slots, peers[j]]
        return pltpu.make_async_remote_copy(
            view, view, fsend_sem, frecv_sem, device_id={"sh": partner}, device_id_type=MESH)

    def pack(c, j):
        first = chips[j] * GRAINS + jnp.where(c >= steps, c - steps, c) * (CSLOTS // GRAIN)
        slot = lax.rem(c, AHEAD)

        def piece(i, _):
            entry = tab_ref[first + i]
            at = lax.div(entry, 64)
            plain = rows[j][pl.ds(at, GRAIN)]
            wrapped = rows[j][pl.ds(jnp.minimum(at + WINDOW, CHIP_ROWS * SEQ - GRAIN), GRAIN)]
            pos = lax.broadcasted_iota(jnp.int32, (GRAIN, 2, HD), 0)
            stage[j, slot, pl.ds(i * GRAIN, GRAIN)] = jnp.where(pos < lax.rem(entry, 64), wrapped, plain)
            return 0
        lax.fori_loop(0, CSLOTS // GRAIN, piece, 0)

    def normalize():
        x = x_ref[...].astype(jnp.float32)
        inv_rms = lax.rsqrt(jnp.mean(x * x, axis=-1, keepdims=True) + EPS)
        normed[...] = (x * inv_rms * g_ref[...].astype(jnp.float32).reshape(1, -1)).astype(jnp.bfloat16)

    def project(first):
        def step(k, _):
            i = first + k
            for ref, lo, hi in ((wq_ref, 0, 16), (wk_ref, 16, 24), (wv_ref, 24, 32)):
                @pl.when(jnp.logical_and(k < WPART, jnp.logical_and(i >= lo, i < hi)))
                def _():
                    cols = pl.ds(pl.multiple_of((i - lo) * WCOLS, WCOLS), WCOLS)
                    pltpu.make_async_copy(ref.at[:, cols], wbuf.at[lax.rem(i, WBUF)], w_sem.at[lax.rem(i, WBUF)]).start()
            e = i - (WBUF - 1)

            @pl.when(k >= WBUF - 1)
            def _():
                slot = lax.rem(e, WBUF)
                pltpu.make_async_copy(wq_ref.at[:, pl.ds(0, WCOLS)], wbuf.at[slot], w_sem.at[slot]).wait()

                def part(kk, y):
                    at = pl.ds(pl.multiple_of(kk * KSTEP, KSTEP), KSTEP)
                    return y + jnp.dot(normed[:, at], wbuf[slot, at], preferred_element_type=jnp.float32)
                y = lax.fori_loop(0, 4608 // KSTEP, part, jnp.zeros((2, WCOLS), jnp.float32))
                p_ref[:, pl.ds(pl.multiple_of(e * WCOLS, WCOLS), WCOLS)] = y.astype(jnp.bfloat16)
            return 0
        lax.fori_loop(0, WPART + WBUF - 1, step, 0)

    def body(t, _):
        for j in range(4):
            c = t - LAGS[j]
            u = c - AHEAD

            @pl.when(jnp.logical_and(u >= 0, u < total))
            def _():
                if j < 3:
                    send(u, j).wait_send()
                else:
                    own(u).wait()
                    forward(u, 3).start()

            @pl.when(jnp.logical_and(c >= 0, c < total))
            def _():
                @pl.when(jnp.logical_or(c == 0, c == steps))
                def _():
                    load(k_ref, j).wait()

                if j < 2:
                    @pl.when(c == 0)
                    def _():
                        for i in ((1, 2) if j == 0 else (3,)):
                            load(k_ref, i).start()
                pack(c, j)

                @pl.when(c == steps - 1)
                def _():
                    load(v_ref, j).start()
                if j < 3:
                    send(c, j).start()
                else:
                    own(c).start()

        @pl.when(t == 6)
        def _():
            normalize()

        @pl.when(jnp.logical_and(lax.rem(t, 8) == 7, t < 32))
        def _():
            project(t - 7)

        for j in range(3):
            u = t - LAGS[j] - AHEAD

            @pl.when(jnp.logical_and(u >= 0, u < total))
            def _():
                send(u, j).wait_recv()
                forward(u, j).start()
        return 0
    lax.fori_loop(0, total + AHEAD + LAGS[3], body, 0)

    view = r_ref.at[:, pl.ds(0, steps * CSLOTS), pl.ds(0, 4)]
    everything = pltpu.make_async_remote_copy(
        view, view, fsend_sem, frecv_sem, device_id={"sh": partner}, device_id_type=MESH)
    everything.wait()


def exchange(level, table, x, g, k, v, wq, wk, wv):
    hbm = pl.BlockSpec(memory_space=pl.ANY)
    vmem = pl.BlockSpec(memory_space=pltpu.VMEM)
    smem = pl.BlockSpec(memory_space=pltpu.SMEM)
    rows = pltpu.VMEM((CHIP_ROWS * SEQ, 2, HD), jnp.bfloat16)

    def branch(i, *args):
        return pl.pallas_call(
            functools.partial(exchange_kernel, LEVELS[i]),
            out_shape=(jax.ShapeDtypeStruct((2, CHIP_ROWS * WINDOW + BLK, 8, 2, HD), jnp.bfloat16),
                       jax.ShapeDtypeStruct((2, 8192), jnp.bfloat16)),
            in_specs=[smem, vmem, vmem] + [hbm] * 5,
            out_specs=(hbm, vmem),
            scratch_shapes=[
                rows, rows, rows, rows,
                pltpu.VMEM((4, AHEAD, CSLOTS, 2, HD), jnp.bfloat16),
                pltpu.VMEM((WBUF, 4608, WCOLS), jnp.bfloat16),
                pltpu.VMEM((2, 4608), jnp.bfloat16),
                pltpu.SemaphoreType.DMA((4,)),
                pltpu.SemaphoreType.DMA((3, AHEAD)), pltpu.SemaphoreType.DMA((3, ARRIVE)),
                pltpu.SemaphoreType.DMA((AHEAD,)),
                pltpu.SemaphoreType.DMA, pltpu.SemaphoreType.DMA,
                pltpu.SemaphoreType.DMA((WBUF,)),
            ],
            compiler_params=pltpu.CompilerParams(
                collective_id=i, has_side_effects=True, vmem_limit_bytes=62 * 2**20),
            name=f"exchange_{LEVELS[i]}",
        )(*args)
    return lax.switch(level, [functools.partial(branch, i) for i in range(len(LEVELS))],
                      table, x, g, k.reshape(BATCH * SEQ, 2, HD), v.reshape(BATCH * SEQ, 2, HD), wq, wk, wv)


NBUF = 8
LOOK = 5
COLS = BLK * KVH


def attend_kernel(len_ref, q_ref, kn_ref, vn_ref, r_ref, o_ref, kc_ref, vc_ref,
                  buf, zbuf, sc, mx, acc, in_sem, out_sem, zero_sem):
    me = lax.axis_index("sh")
    row0 = 2 * me
    base = CHIP_ROWS * (me // 2)
    lens = [len_ref[row0], len_ref[row0 + 1]]
    before = row_grains(len_ref[base]) + row_grains(len_ref[base + 1])
    start0 = jnp.where(me % 2 == 1, before, 0)
    starts = [start0, start0 + row_grains(lens[0])]
    acts = [jnp.where(n >= WINDOW, NBLK, n // BLK + 1) for n in lens]
    units = acts[0] + acts[1]

    def where_is(u):
        second = u >= acts[0]
        r = second.astype(jnp.int32)
        sig = jnp.where(second, u - acts[0], u)
        at = jnp.where(second, starts[1], starts[0]) * GRAIN + sig * BLK
        return r, sig, at, jnp.where(second, lens[1], lens[0])

    def in_copy(half, w, u):
        _, _, at, _ = where_is(u)
        return pltpu.make_async_copy(r_ref.at[half, pl.ds(at, BLK)], buf.at[w % NBUF], in_sem.at[w % NBUF])

    def out_copy(ref, w, u):
        r, sig, _, _ = where_is(u)
        return pltpu.make_async_copy(buf.at[w % NBUF], ref.at[r, pl.ds(sig * BLK, BLK)], out_sem.at[w % NBUF])

    def start_in(w):
        @pl.when(w < units)
        def _():
            in_copy(0, w, w).start()

        @pl.when(jnp.logical_and(w >= units, w < 2 * units))
        def _():
            in_copy(1, w, w - units).start()

    def wait_out(w):
        @pl.when(w >= 0)
        def _():
            out_copy(kc_ref, w, 0).wait()

    for w in range(LOOK):
        start_in(jnp.int32(w))

    zbuf[...] = jnp.zeros_like(zbuf)

    def zero_copies(r, sig):
        return [pltpu.make_async_copy(zbuf, ref.at[r, pl.ds(sig * BLK, BLK)], zero_sem.at[x])
                for x, ref in enumerate((kc_ref, vc_ref))]
    for r in range(2):
        def put_zero(sig, _, r=r):
            for c in zero_copies(r, sig):
                c.start()
            return 0
        lax.fori_loop(acts[r], NBLK, put_zero, 0)

    mx[...] = jnp.full_like(mx, -jnp.inf)
    acc[...] = jnp.zeros_like(acc)
    col = lax.broadcasted_iota(jnp.int32, (32, COLS), 1)
    rowid = lax.broadcasted_iota(jnp.int32, (32, COLS), 0)
    match = (rowid % KVH) == (col % KVH)
    col2 = lax.broadcasted_iota(jnp.int32, (2, COLS), 1) // KVH
    scale = 1.0 / HD ** 0.5

    def fix(slot, r, sig, n, new_ref):
        new_slot = n % WINDOW

        @pl.when(sig == new_slot // BLK)
        def _():
            here = sig * BLK + lax.broadcasted_iota(jnp.int32, (BLK, KVH, HD), 0)
            val = buf[slot]
            val = jnp.where(here > n, jnp.zeros_like(val), val)
            new = jnp.broadcast_to(new_ref[r][None], val.shape)
            buf[slot] = jnp.where(here == new_slot, new, val)

    def k_step(u, _):
        r, sig, _, n = where_is(u)
        slot = u % NBUF
        wait_out(u + LOOK - NBUF)
        start_in(u + LOOK)
        in_copy(0, u, u).wait()
        fix(slot, r, sig, n, kn_ref)
        kb = buf[slot].reshape(COLS, HD)
        s = lax.dot_general(q_ref[r], kb, (((1,), (1,)), ((), ())), preferred_element_type=jnp.float32)
        out_copy(kc_ref, u, u).start()
        s = jnp.where(match, s, 0.0)
        s = jnp.concatenate([jnp.sum(s[:KVH], axis=0, keepdims=True),
                             jnp.sum(s[KVH:], axis=0, keepdims=True)], axis=0)
        s = jnp.where(sig * BLK + col2 > n, -jnp.inf, s * scale)
        sc[u] = s
        mx[r] = jnp.maximum(mx[r], s)
        return 0
    lax.fori_loop(0, units, k_step, 0)

    def fold(x, op):
        y = x[:, :HD]
        for i in range(1, COLS // HD):
            y = op(y, x[:, i * HD:(i + 1) * HD])
        for sh in (16, 32, 64):
            y = op(y, pltpu.roll(y, sh, 1))
        return jnp.concatenate([y] * (COLS // HD), axis=1)

    for r in range(2):
        top = fold(mx[r], jnp.maximum)
        lo = 0 if r == 0 else acts[0]

        def exp_step(i, tot, top=top, lo=lo):
            e = jnp.exp(sc[lo + i] - top)
            sc[lo + i] = e
            return tot + e
        tot = lax.fori_loop(0, acts[r], exp_step, jnp.zeros((2, COLS), jnp.float32))
        mx[r] = fold(tot, jnp.add)

    def v_step(u, _):
        r, sig, _, n = where_is(u)
        w = u + units
        slot = w % NBUF
        wait_out(w + LOOK - NBUF)
        start_in(w + LOOK)
        in_copy(1, w, u).wait()
        fix(slot, r, sig, n, vn_ref)
        p = sc[u] / mx[r]
        wide = jnp.concatenate([jnp.broadcast_to(p[0:1], (KVH, COLS)),
                                jnp.broadcast_to(p[1:2], (KVH, COLS))], axis=0)
        wide = jnp.where(match, wide, 0.0).astype(jnp.bfloat16)
        vb = buf[slot].reshape(COLS, HD)
        acc[r] += jnp.dot(wide, vb, preferred_element_type=jnp.float32)
        out_copy(vc_ref, w, u).start()
        return 0
    lax.fori_loop(0, units, v_step, 0)
    o_ref[...] = acc[...].astype(o_ref.dtype)

    def drain(w, _):
        wait_out(w)
        return 0
    lax.fori_loop(2 * units + LOOK - NBUF, 2 * units, drain, 0)
    for r in range(2):
        def wait_zero(sig, _, r=r):
            for c in zero_copies(r, sig):
                c.wait()
            return 0
        lax.fori_loop(acts[r], NBLK, wait_zero, 0)


def attend(lengths, q, kn, vn, r):
    hbm = pl.BlockSpec(memory_space=pl.ANY)
    vmem = pl.BlockSpec(memory_space=pltpu.VMEM)
    cache = jax.ShapeDtypeStruct((2, WINDOW, KVH, HD), jnp.bfloat16)
    return pl.pallas_call(
        attend_kernel,
        out_shape=(jax.ShapeDtypeStruct((2, 32, HD), jnp.bfloat16), cache, cache),
        in_specs=[pl.BlockSpec(memory_space=pltpu.SMEM), vmem, vmem, vmem, hbm],
        out_specs=(vmem, hbm, hbm),
        scratch_shapes=[
            pltpu.VMEM((NBUF, BLK, KVH, HD), jnp.bfloat16),
            pltpu.VMEM((BLK, KVH, HD), jnp.bfloat16),
            pltpu.VMEM((2 * NBLK, 2, COLS), jnp.float32),
            pltpu.VMEM((2, 2, COLS), jnp.float32),
            pltpu.VMEM((2, 32, HD), jnp.float32),
            pltpu.SemaphoreType.DMA((NBUF,)), pltpu.SemaphoreType.DMA((NBUF,)),
            pltpu.SemaphoreType.DMA((2,)),
        ],
        name="attend",
    )(lengths, q, kn, vn, r.reshape(2, CHIP_ROWS * WINDOW + BLK, KVH, HD))


def rotate(heads, positions):
    half = HD // 2
    inv_freq = THETA ** (-2.0 * jnp.arange(half, dtype=jnp.float32) / HD)
    angles = positions.astype(jnp.float32).reshape(positions.shape + (1,) * (heads.ndim - 1)) * inv_freq
    cos_part = jnp.cos(angles)
    sin_part = jnp.sin(angles)
    first = heads[..., :half].astype(jnp.float32)
    second = heads[..., half:].astype(jnp.float32)
    return jnp.concatenate([first * cos_part - second * sin_part, second * cos_part + first * sin_part], axis=-1).astype(jnp.bfloat16)


def solution(mesh):
    head_spec = P('dp', None, 'sh', None)
    row_spec = P(('dp', 'sh'))
    full_spec = P(None, None)

    def per_device(k_prefill, v_prefill, lengths, residual, norm_gain, w_query, w_key, w_value, w_out):
        rows = residual.shape[0]
        mine = lax.dynamic_slice_in_dim(lengths, lax.axis_index('sh') * rows, rows)
        longest = jnp.max(jnp.sum(row_grains(lengths).reshape(4, CHIP_ROWS), axis=1)) * GRAIN
        level = jnp.sum(longest > jnp.asarray(LEVELS, jnp.int32) * CSLOTS).astype(jnp.int32)
        r, p = exchange(level, source_table(lengths), residual, norm_gain, k_prefill, v_prefill, w_query, w_key, w_value)
        q = p[:, :4096].reshape(rows, KVH, 2, HD)
        kn = p[:, 4096:6144].reshape(rows, KVH, HD)
        vn = p[:, 6144:].reshape(rows, KVH, HD)
        q = rotate(q, mine).transpose(0, 2, 1, 3).reshape(rows, 2 * KVH, HD)
        kn = rotate(kn, mine)
        o, kc, vc = attend(lengths, q, kn, vn, r)
        o = o.reshape(rows, 2, KVH, HD).transpose(0, 2, 1, 3).reshape(rows, 2 * KVH * HD)
        out = (residual.astype(jnp.float32) + jnp.dot(o, w_out, preferred_element_type=jnp.float32)).astype(jnp.bfloat16)
        return out, kc, vc
    return jax.shard_map(per_device, mesh=mesh, in_specs=(head_spec, head_spec, P('dp'), P(('dp', 'sh'), None), P(None), full_spec, full_spec, full_spec, full_spec), out_specs=(P(('dp', 'sh'), None), row_spec, row_spec), check_vma=False)
```

```python
import functools

import jax
import jax.numpy as jnp
from jax import lax
from jax.experimental import pallas as pl
from jax.experimental.pallas import tpu as pltpu
from jax.sharding import PartitionSpec as P

WINDOW = 4096
SEQ = 5120
BATCH = 16
KVH = 16
HD = 128
THETA = 10000.0
EPS = 1e-5
MESH = pl.DeviceIdType.MESH

BLK = 128
NBLK = WINDOW // BLK
CHIP_ROWS = 4
GRAIN = 32
GRAINS = CHIP_ROWS * WINDOW // GRAIN
CSLOTS = 256
MAXCHUNKS = CHIP_ROWS * WINDOW // CSLOTS
HEAD = 1024
HEADG = HEAD // GRAIN
CHUNKG = CSLOTS // GRAIN
LEVELS = (24, 30, 34) + tuple(range(37, 60)) + (61, MAXCHUNKS)
AHEAD = 8
ARRIVE = 32
LAGS = (0, 2, 3, 7)
WCOLS = 256
WBUF = 4
WPART = 8
KSTEP = 512


def row_grains(n):
    return (jnp.minimum(n, WINDOW) + (GRAIN - 1)) // GRAIN


def first_row_rest(n):
    count = row_grains(n)
    return jnp.minimum(count, HEADG) + jnp.maximum(count - HEADG - CHUNKG, 0)


def prepare_kernel(len_ref, tab_ref, level_ref):
    shape = (GRAINS // HD, HD)
    grain = lax.broadcasted_iota(jnp.int32, shape, 0) * HD + lax.broadcasted_iota(jnp.int32, shape, 1)
    longest = jnp.int32(0)
    for c in range(4):
        n = [len_ref[c * CHIP_ROWS + r] for r in range(CHIP_ROWS)]
        begin = CHUNKG + first_row_rest(n[0])
        at = jnp.where(grain < CHUNKG, grain + HEADG, jnp.where(grain < CHUNKG + HEADG, grain - CHUNKG, grain))
        place = jnp.zeros(shape, jnp.int32)
        length = jnp.full(shape, n[0], jnp.int32)
        for r in range(1, CHIP_ROWS):
            after = grain >= begin
            at = jnp.where(after, grain - begin, at)
            place = jnp.where(after, r * SEQ, place)
            length = jnp.where(after, n[r], length)
            begin = begin + row_grains(n[r])
        longest = jnp.maximum(longest, begin)
        at = jnp.minimum(at * GRAIN, WINDOW - GRAIN)
        wrapped = jnp.minimum(jnp.maximum(length - WINDOW - at, 0), GRAIN)
        tab_ref[pl.ds(c * shape[0], shape[0])] = (place + at) * 64 + wrapped
    level = jnp.int32(0)
    for lv in LEVELS:
        level += (longest * GRAIN > lv * CSLOTS).astype(jnp.int32)
    level_ref[0] = level


def prepare(lengths):
    smem = pl.BlockSpec(memory_space=pltpu.SMEM)
    return pl.pallas_call(
        prepare_kernel,
        out_shape=(jax.ShapeDtypeStruct((4 * GRAINS // HD, HD), jnp.int32), jax.ShapeDtypeStruct((1,), jnp.int32)),
        in_specs=[smem],
        out_specs=(pl.BlockSpec(memory_space=pltpu.VMEM), smem),
        name="prepare",
    )(lengths)


def exchange_kernel(steps, tab_ref, x_ref, g_ref, k_ref, v_ref, wq_ref, wk_ref, wv_ref,
                    r_ref, p_ref, rows0, rows1, rows2, rows3, stage, wbuf, normed,
                    load_sem, send_sem, recv_sem, own_sem, fsend_sem, frecv_sem, w_sem):
    me = lax.axis_index("sh")
    core = lax.rem(me, 2)
    my_chip = lax.div(me, 2)
    chip_x = lax.rem(my_chip, 2)
    chip_y = lax.div(my_chip, 2)
    partner = me + 1 - 2 * core
    chips = ((1 - chip_y) * 2 + (1 - chip_x), (1 - chip_y) * 2 + chip_x, chip_y * 2 + (1 - chip_x), my_chip)
    peers = [c * 2 + core for c in chips]
    rows = (rows0, rows1, rows2, rows3)
    total = 2 * steps

    def load(ref, j):
        flat = CHIP_ROWS * SEQ
        return pltpu.make_async_copy(ref.at[pl.ds(chips[j] * flat, flat)], rows[j], load_sem.at[j])

    load(k_ref, 0).start()
    sent_first = pl.ds(0, CSLOTS)
    barrier = pltpu.get_barrier_semaphore()
    for p in peers[:3] + [partner]:
        pl.semaphore_signal(barrier, inc=1, device_id={"sh": p}, device_id_type=MESH)
    pl.semaphore_wait(barrier, 4)

    def place(c):
        phase = (c >= steps).astype(jnp.int32)
        return phase, pl.ds((c - phase * steps) * CSLOTS, CSLOTS), lax.rem(c, AHEAD)

    def send(c, j):
        phase, slots, slot = place(c)
        return pltpu.make_async_remote_copy(
            stage.at[j, slot], r_ref.at[phase, slots, me], send_sem.at[j, slot], recv_sem.at[j, lax.rem(c, ARRIVE)],
            device_id={"sh": peers[j]}, device_id_type=MESH)

    for j in range(3):
        pltpu.make_async_remote_copy(
            k_ref.at[pl.ds(chips[j] * (CHIP_ROWS * SEQ) + HEAD, CSLOTS)], r_ref.at[0, sent_first, me],
            send_sem.at[j, 0], recv_sem.at[j, 0], device_id={"sh": peers[j]}, device_id_type=MESH).start()

    def own(c):
        phase, slots, slot = place(c)
        return pltpu.make_async_copy(stage.at[3, slot], r_ref.at[phase, slots, me], own_sem.at[slot])

    def forward(c, j):
        phase, slots, _ = place(c)
        view = r_ref.at[phase, slots, peers[j]]
        return pltpu.make_async_remote_copy(
            view, view, fsend_sem, frecv_sem, device_id={"sh": partner}, device_id_type=MESH)

    def pack(c, j):
        first = chips[j] * GRAINS + jnp.where(c >= steps, c - steps, c) * (CSLOTS // GRAIN)
        slot = lax.rem(c, AHEAD)

        def piece(i, _):
            grain = first + i
            entry = tab_ref[lax.div(grain, HD), lax.rem(grain, HD)]
            at = lax.div(entry, 64)
            plain = rows[j][pl.ds(at, GRAIN)]
            wrapped = rows[j][pl.ds(jnp.minimum(at + WINDOW, CHIP_ROWS * SEQ - GRAIN), GRAIN)]
            pos = lax.broadcasted_iota(jnp.int32, (GRAIN, 2, HD), 0)
            stage[j, slot, pl.ds(i * GRAIN, GRAIN)] = jnp.where(pos < lax.rem(entry, 64), wrapped, plain)
            return 0
        lax.fori_loop(0, CSLOTS // GRAIN, piece, 0)

    def normalize():
        x = x_ref[...].astype(jnp.float32)
        inv_rms = lax.rsqrt(jnp.mean(x * x, axis=-1, keepdims=True) + EPS)
        normed[...] = (x * inv_rms * g_ref[...].astype(jnp.float32).reshape(1, -1)).astype(jnp.bfloat16)

    def project(first):
        def step(k, _):
            i = first + k
            for ref, lo, hi in ((wq_ref, 0, 16), (wk_ref, 16, 24), (wv_ref, 24, 32)):
                @pl.when(jnp.logical_and(k < WPART, jnp.logical_and(i >= lo, i < hi)))
                def _():
                    cols = pl.ds(pl.multiple_of((i - lo) * WCOLS, WCOLS), WCOLS)
                    pltpu.make_async_copy(ref.at[:, cols], wbuf.at[lax.rem(i, WBUF)], w_sem.at[lax.rem(i, WBUF)]).start()
            e = i - (WBUF - 1)

            @pl.when(k >= WBUF - 1)
            def _():
                slot = lax.rem(e, WBUF)
                pltpu.make_async_copy(wq_ref.at[:, pl.ds(0, WCOLS)], wbuf.at[slot], w_sem.at[slot]).wait()

                def part(kk, y):
                    at = pl.ds(pl.multiple_of(kk * KSTEP, KSTEP), KSTEP)
                    return y + jnp.dot(normed[:, at], wbuf[slot, at], preferred_element_type=jnp.float32)
                y = lax.fori_loop(0, 4608 // KSTEP, part, jnp.zeros((2, WCOLS), jnp.float32))
                p_ref[:, pl.ds(pl.multiple_of(e * WCOLS, WCOLS), WCOLS)] = y.astype(jnp.bfloat16)
            return 0
        lax.fori_loop(0, WPART + WBUF - 1, step, 0)

    def body(t, _):
        for j in range(4):
            c = t - LAGS[j]
            u = c - AHEAD

            @pl.when(jnp.logical_and(u >= 0, u < total))
            def _():
                if j < 3:
                    send(u, j).wait_send()
                else:
                    own(u).wait()
                    forward(u, 3).start()

            @pl.when(jnp.logical_and(c >= 0, c < total))
            def _():
                @pl.when(jnp.logical_or(c == 0, c == steps))
                def _():
                    load(k_ref, j).wait()

                if j < 2:
                    @pl.when(c == 0)
                    def _():
                        for i in ((1, 2) if j == 0 else (3,)):
                            load(k_ref, i).start()

                @pl.when(c > (0 if j < 3 else -1))
                def _():
                    pack(c, j)
                    if j < 3:
                        send(c, j).start()
                    else:
                        own(c).start()

                @pl.when(c == steps - 1)
                def _():
                    load(v_ref, j).start()

        @pl.when(t == 6)
        def _():
            normalize()

        @pl.when(jnp.logical_and(lax.rem(t, 8) == 7, t < 32))
        def _():
            project(t - 7)

        for j in range(3):
            u = t - LAGS[j] - AHEAD

            @pl.when(jnp.logical_and(u >= 0, u < total))
            def _():
                send(u, j).wait_recv()
                forward(u, j).start()
        return 0
    lax.fori_loop(0, total + AHEAD + LAGS[3], body, 0)

    view = r_ref.at[:, pl.ds(0, steps * CSLOTS), pl.ds(0, 4)]
    everything = pltpu.make_async_remote_copy(
        view, view, fsend_sem, frecv_sem, device_id={"sh": partner}, device_id_type=MESH)
    everything.wait()


def exchange(level, table, x, g, k, v, wq, wk, wv):
    hbm = pl.BlockSpec(memory_space=pl.ANY)
    vmem = pl.BlockSpec(memory_space=pltpu.VMEM)
    smem = pl.BlockSpec(memory_space=pltpu.SMEM)
    rows = pltpu.VMEM((CHIP_ROWS * SEQ, 2, HD), jnp.bfloat16)

    def branch(i, *args):
        return pl.pallas_call(
            functools.partial(exchange_kernel, LEVELS[i]),
            out_shape=(jax.ShapeDtypeStruct((2, CHIP_ROWS * WINDOW + BLK, 8, 2, HD), jnp.bfloat16),
                       jax.ShapeDtypeStruct((2, 8192), jnp.bfloat16)),
            in_specs=[smem, vmem, vmem] + [hbm] * 5,
            out_specs=(hbm, vmem),
            scratch_shapes=[
                rows, rows, rows, rows,
                pltpu.VMEM((4, AHEAD, CSLOTS, 2, HD), jnp.bfloat16),
                pltpu.VMEM((WBUF, 4608, WCOLS), jnp.bfloat16),
                pltpu.VMEM((2, 4608), jnp.bfloat16),
                pltpu.SemaphoreType.DMA((4,)),
                pltpu.SemaphoreType.DMA((3, AHEAD)), pltpu.SemaphoreType.DMA((3, ARRIVE)),
                pltpu.SemaphoreType.DMA((AHEAD,)),
                pltpu.SemaphoreType.DMA, pltpu.SemaphoreType.DMA,
                pltpu.SemaphoreType.DMA((WBUF,)),
            ],
            compiler_params=pltpu.CompilerParams(
                collective_id=i, has_side_effects=True, vmem_limit_bytes=62 * 2**20),
            name=f"exchange_{LEVELS[i]}",
        )(*args)
    return lax.switch(level, [functools.partial(branch, i) for i in range(len(LEVELS))],
                      table, x, g, k.reshape(BATCH * SEQ, 2, HD), v.reshape(BATCH * SEQ, 2, HD), wq, wk, wv)


NBUF = 16
LOOK = 10
COLS = BLK * KVH


def attend_kernel(len_ref, p_ref, cos_ref, sin_ref, r_ref, o_ref, kc_ref, vc_ref,
                  q_ref, kn_ref, vn_ref, buf, zbuf, sc, mx, acc, in_sem, out_sem, zero_sem):
    me = lax.axis_index("sh")
    row0 = 2 * me
    base = CHIP_ROWS * (me // 2)
    lens = [len_ref[row0], len_ref[row0 + 1]]
    odd = me % 2 == 1
    start0 = jnp.where(odd, CHUNKG + first_row_rest(len_ref[base]) + row_grains(len_ref[base + 1]), 0)
    starts = [start0, jnp.where(odd, start0 + row_grains(lens[0]), CHUNKG + first_row_rest(lens[0]))]
    acts = [jnp.where(n >= WINDOW, NBLK, n // BLK + 1) for n in lens]
    units = acts[0] + acts[1]

    def where_is(u):
        second = u >= acts[0]
        r = second.astype(jnp.int32)
        sig = jnp.where(second, u - acts[0], u)
        at = jnp.where(second, starts[1], starts[0]) * GRAIN + sig * BLK
        opening = jnp.where(sig < HEAD // BLK, sig * BLK + CSLOTS,
                            jnp.where(sig < (HEAD + CSLOTS) // BLK, sig * BLK - HEAD, sig * BLK))
        at = jnp.where(jnp.logical_or(odd, second), at, opening)
        return r, sig, at, jnp.where(second, lens[1], lens[0])

    def in_copy(half, w, u):
        _, _, at, _ = where_is(u)
        return pltpu.make_async_copy(r_ref.at[half, pl.ds(at, BLK)], buf.at[w % NBUF], in_sem.at[w % NBUF])

    def out_copy(ref, w, u):
        r, sig, _, _ = where_is(u)
        return pltpu.make_async_copy(buf.at[w % NBUF], ref.at[r, pl.ds(sig * BLK, BLK)], out_sem.at[w % NBUF])

    def start_in(w):
        @pl.when(w < units)
        def _():
            in_copy(0, w, w).start()

        @pl.when(jnp.logical_and(w >= units, w < 2 * units))
        def _():
            in_copy(1, w, w - units).start()

    def wait_out(w):
        @pl.when(w >= 0)
        def _():
            out_copy(kc_ref, w, 0).wait()

    for w in range(LOOK):
        start_in(jnp.int32(w))

    zbuf[...] = jnp.zeros_like(zbuf)

    def zero_copies(r, sig):
        return [pltpu.make_async_copy(zbuf, ref.at[r, pl.ds(sig * BLK, BLK)], zero_sem.at[x])
                for x, ref in enumerate((kc_ref, vc_ref))]
    for r in range(2):
        def put_zero(sig, _, r=r):
            for c in zero_copies(r, sig):
                c.start()
            return 0
        lax.fori_loop(acts[r], NBLK, put_zero, 0)

    p = p_ref[...].astype(jnp.float32)
    for r in range(2):
        heads = [p[r:r + 1, h * HD:(h + 1) * HD] for h in range(64)]
        cos, sin = cos_ref[r:r + 1], sin_ref[r:r + 1]

        def turned(x):
            return (x * cos + pltpu.roll(x, HD // 2, 1) * sin).astype(jnp.bfloat16)
        q_ref[r] = turned(jnp.concatenate(heads[0:32:2] + heads[1:32:2], axis=0))
        kn_ref[r] = turned(jnp.concatenate(heads[32:48], axis=0))
        vn_ref[r] = jnp.concatenate(heads[48:64], axis=0).astype(jnp.bfloat16)

    mx[...] = jnp.full_like(mx, -jnp.inf)
    acc[...] = jnp.zeros_like(acc)
    col = lax.broadcasted_iota(jnp.int32, (32, COLS), 1)
    rowid = lax.broadcasted_iota(jnp.int32, (32, COLS), 0)
    match = (rowid % KVH) == (col % KVH)
    col2 = lax.broadcasted_iota(jnp.int32, (2, COLS), 1) // KVH
    scale = 1.0 / HD ** 0.5

    def fix(slot, r, sig, n, new_ref):
        new_slot = n % WINDOW

        @pl.when(sig == new_slot // BLK)
        def _():
            here = sig * BLK + lax.broadcasted_iota(jnp.int32, (BLK, KVH, HD), 0)
            val = buf[slot]
            val = jnp.where(here > n, jnp.zeros_like(val), val)
            new = jnp.broadcast_to(new_ref[r][None], val.shape)
            buf[slot] = jnp.where(here == new_slot, new, val)

    def k_step(u, _):
        r, sig, _, n = where_is(u)
        slot = u % NBUF
        wait_out(u + LOOK - NBUF)
        start_in(u + LOOK)
        in_copy(0, u, u).wait()
        fix(slot, r, sig, n, kn_ref)
        kb = buf[slot].reshape(COLS, HD)
        s = lax.dot_general(q_ref[r], kb, (((1,), (1,)), ((), ())), preferred_element_type=jnp.float32)
        out_copy(kc_ref, u, u).start()
        s = jnp.where(match, s, 0.0)
        s = jnp.concatenate([jnp.sum(s[:KVH], axis=0, keepdims=True),
                             jnp.sum(s[KVH:], axis=0, keepdims=True)], axis=0)
        s = jnp.where(sig * BLK + col2 > n, -jnp.inf, s * scale)
        sc[u] = s
        mx[r] = jnp.maximum(mx[r], s)
        return 0
    lax.fori_loop(0, units, k_step, 0)

    def fold(x, op):
        y = x[:, :HD]
        for i in range(1, COLS // HD):
            y = op(y, x[:, i * HD:(i + 1) * HD])
        for sh in (16, 32, 64):
            y = op(y, pltpu.roll(y, sh, 1))
        return jnp.concatenate([y] * (COLS // HD), axis=1)

    for r in range(2):
        top = fold(mx[r], jnp.maximum)
        lo = 0 if r == 0 else acts[0]

        def exp_step(i, tot, top=top, lo=lo):
            e = jnp.exp(sc[lo + i] - top)
            sc[lo + i] = e
            return tot + e
        tot = lax.fori_loop(0, acts[r], exp_step, jnp.zeros((2, COLS), jnp.float32))
        mx[r] = fold(tot, jnp.add)

    def v_step(u, _):
        r, sig, _, n = where_is(u)
        w = u + units
        slot = w % NBUF
        wait_out(w + LOOK - NBUF)
        start_in(w + LOOK)
        in_copy(1, w, u).wait()
        fix(slot, r, sig, n, vn_ref)
        p = sc[u] / mx[r]
        wide = jnp.concatenate([jnp.broadcast_to(p[0:1], (KVH, COLS)),
                                jnp.broadcast_to(p[1:2], (KVH, COLS))], axis=0)
        wide = jnp.where(match, wide, 0.0).astype(jnp.bfloat16)
        vb = buf[slot].reshape(COLS, HD)
        acc[r] += jnp.dot(wide, vb, preferred_element_type=jnp.float32)
        out_copy(vc_ref, w, u).start()
        return 0
    lax.fori_loop(0, units, v_step, 0)
    for h in range(32):
        o_ref[:, h * HD:(h + 1) * HD] = acc[:, (h % 2) * KVH + h // 2].astype(o_ref.dtype)

    def drain(w, _):
        wait_out(w)
        return 0
    lax.fori_loop(2 * units + LOOK - NBUF, 2 * units, drain, 0)
    for r in range(2):
        def wait_zero(sig, _, r=r):
            for c in zero_copies(r, sig):
                c.wait()
            return 0
        lax.fori_loop(acts[r], NBLK, wait_zero, 0)


def attend(lengths, p, cos, sin, r):
    hbm = pl.BlockSpec(memory_space=pl.ANY)
    vmem = pl.BlockSpec(memory_space=pltpu.VMEM)
    cache = jax.ShapeDtypeStruct((2, WINDOW, KVH, HD), jnp.bfloat16)
    return pl.pallas_call(
        attend_kernel,
        out_shape=(jax.ShapeDtypeStruct((2, 32 * HD), jnp.bfloat16), cache, cache),
        in_specs=[pl.BlockSpec(memory_space=pltpu.SMEM), vmem, vmem, vmem, hbm],
        out_specs=(vmem, hbm, hbm),
        scratch_shapes=[
            pltpu.VMEM((2, 32, HD), jnp.bfloat16),
            pltpu.VMEM((2, KVH, HD), jnp.bfloat16),
            pltpu.VMEM((2, KVH, HD), jnp.bfloat16),
            pltpu.VMEM((NBUF, BLK, KVH, HD), jnp.bfloat16),
            pltpu.VMEM((BLK, KVH, HD), jnp.bfloat16),
            pltpu.VMEM((2 * NBLK, 2, COLS), jnp.float32),
            pltpu.VMEM((2, 2, COLS), jnp.float32),
            pltpu.VMEM((2, 32, HD), jnp.float32),
            pltpu.SemaphoreType.DMA((NBUF,)), pltpu.SemaphoreType.DMA((NBUF,)),
            pltpu.SemaphoreType.DMA((2,)),
        ],
        name="attend",
    )(lengths, p, cos, sin, r.reshape(2, CHIP_ROWS * WINDOW + BLK, KVH, HD))


MODEL = 4608
PCOLS = 640


def first_col(d):
    return lax.div(9 * d, 2) * HD


def project_kernel(o_ref, x_ref, w_ref, out_ref, part, rows, wide, made, back,
                   w_sem, osend_sem, orecv_sem, bsend_sem, brecv_sem):
    me = lax.axis_index("sh")
    mine = pl.ds(pl.multiple_of(first_col(me), HD), PCOLS)
    weights = pltpu.make_async_copy(w_ref.at[:, mine], part, w_sem)
    weights.start()
    others = [lax.rem(me + d, 8) for d in range(1, 8)]
    barrier = pltpu.get_barrier_semaphore()
    for p in others:
        pl.semaphore_signal(barrier, inc=1, device_id={"sh": p}, device_id_type=MESH)
    pl.semaphore_wait(barrier, 7)

    def give(k):
        return pltpu.make_async_remote_copy(
            o_ref, rows.at[me], osend_sem.at[k], orecv_sem.at[k],
            device_id={"sh": others[k]}, device_id_type=MESH)

    def answer(k):
        return pltpu.make_async_remote_copy(
            made.at[others[k]], back.at[me], bsend_sem.at[k], brecv_sem.at[k],
            device_id={"sh": others[k]}, device_id_type=MESH)
    for k in range(7):
        give(k).start()
    rows[me] = o_ref[...]
    weights.wait()
    for k in range(7):
        give(k).wait()
    for i in range(0, 32 * HD, KSTEP):
        wide[:, i:i + KSTEP] = jnp.concatenate(
            [rows[d, :, i:i + KSTEP].astype(jnp.float32) for d in range(8)], axis=0).astype(jnp.bfloat16)

    def step(i, y):
        at = pl.ds(pl.multiple_of(i * KSTEP, KSTEP), KSTEP)
        return y + jnp.dot(wide[:, at], part[at], preferred_element_type=jnp.float32)
    y = lax.fori_loop(0, 32 * HD // KSTEP, step, jnp.zeros((16, PCOLS), jnp.float32))
    for d in range(8):
        made[d] = y[2 * d:2 * d + 2]
    back[me] = made[me]
    for k in range(7):
        answer(k).start()
    for k in range(7):
        answer(k).wait()
    for d in range(8):
        lo = 9 * d // 2 * HD
        cols = slice(lo, min(9 * (d + 1) // 2 * HD, MODEL))
        out_ref[:, cols] = (x_ref[:, cols].astype(jnp.float32) + back[d, :, :cols.stop - lo]).astype(out_ref.dtype)


def project_out(o, x, w):
    vmem = pl.BlockSpec(memory_space=pltpu.VMEM)
    return pl.pallas_call(
        project_kernel,
        out_shape=jax.ShapeDtypeStruct((2, MODEL), jnp.bfloat16),
        in_specs=[vmem, vmem, pl.BlockSpec(memory_space=pl.ANY)],
        out_specs=vmem,
        scratch_shapes=[
            pltpu.VMEM((32 * HD, PCOLS), jnp.bfloat16),
            pltpu.VMEM((8, 2, 32 * HD), jnp.bfloat16),
            pltpu.VMEM((16, 32 * HD), jnp.bfloat16),
            pltpu.VMEM((8, 2, PCOLS), jnp.float32),
            pltpu.VMEM((8, 2, PCOLS), jnp.float32),
            pltpu.SemaphoreType.DMA,
            pltpu.SemaphoreType.DMA((7,)), pltpu.SemaphoreType.DMA((7,)),
            pltpu.SemaphoreType.DMA((7,)), pltpu.SemaphoreType.DMA((7,)),
        ],
        compiler_params=pltpu.CompilerParams(collective_id=len(LEVELS), has_side_effects=True),
        name="project_out",
    )(o, x, w)


def solution(mesh):
    head_spec = P('dp', None, 'sh', None)
    row_spec = P(('dp', 'sh'))
    full_spec = P(None, None)

    def per_device(k_prefill, v_prefill, lengths, residual, norm_gain, w_query, w_key, w_value, w_out):
        rows = residual.shape[0]
        table, level = prepare(lengths)
        r, p = exchange(level[0], table, residual, norm_gain, k_prefill, v_prefill, w_query, w_key, w_value)
        mine = lax.dynamic_slice_in_dim(lengths, lax.axis_index('sh') * rows, rows)
        inv_freq = THETA ** (-2.0 * jnp.arange(HD // 2, dtype=jnp.float32) / HD)
        angles = mine.astype(jnp.float32)[:, None] * inv_freq
        cos = jnp.cos(angles)
        sin = jnp.sin(angles)
        o, kc, vc = attend(lengths, p, jnp.concatenate([cos, cos], axis=1), jnp.concatenate([-sin, sin], axis=1), r)
        return project_out(o, residual, w_out), kc, vc
    return jax.shard_map(per_device, mesh=mesh, in_specs=(head_spec, head_spec, P('dp'), P(('dp', 'sh'), None), P(None), full_spec, full_spec, full_spec, full_spec), out_specs=(P(('dp', 'sh'), None), row_spec, row_spec), check_vma=False)
```
